32 devices in a mesh: replica: 4 (over x, core), fsdp: 8 (over z, y).
Axes of the slice: x: 2, y: 2, z: 4, core: 2. Of those that a mesh axis runs over, the one named last changes fastest.
Arguments:
- deltas: bfloat16 [4, 2, 2048, 16384], P('replica', None, 'fsdp'), may hold values from -3 to 3
- master: float32 [2, 2048, 16384], P(None, 'replica', 'fsdp'), may hold values from -3 to 3
- momentum: float32 [2, 2048, 16384], P(None, 'replica', 'fsdp'), may hold values from -2 to 2
Outputs:
- master_out: float32 [2, 2048, 16384], P(None, 'replica', 'fsdp')
- momentum_out: float32 [2, 2048, 16384], P(None, 'replica', 'fsdp')
- params_out: bfloat16 [2, 2048, 16384], P(None, 'fsdp')
The draws below stay inside these ranges and needn't reach their ends.
All inputs are finite; a program needn't handle non-finite values.
Results may differ from the reference program's by a relative error of at most 0.008.
Values may be sent and summed in bfloat16 or wider, within the bound.
A program may use at most 128 MiB of HBM per device.

```python
import jax
import jax.numpy as jnp

D = 2048
FF = 16384
PROJ = 2
R = 4


def strengthened(result, own_key, source, target, shards_of, factor):
    def block_of(dim):
        return (jnp.arange(result.shape[dim]) // (result.shape[dim] // shards_of)).reshape((-1,) + (1,) * (result.ndim - 1 - dim))

    one_side = jax.random.permutation(own_key, shards_of)[block_of(target)]
    other_side = (block_of(target) + shards_of // 2) % shards_of
    return jnp.where((block_of(source) == one_side) | (block_of(source) == other_side), factor * result, result)


def steps_of(rng, dims, shards, low, high):
    factor_of, own = 1.0, jax.random.fold_in(rng, 6)
    for dim, blocks in shards:
        steps = jnp.exp(jax.random.uniform(jax.random.fold_in(own, dim), (blocks,), jnp.float32, low / len(shards), high / len(shards)))
        factor_of = factor_of * jnp.repeat(steps, dims[dim] // blocks).reshape([-1 if axis == dim else 1 for axis in range(len(dims))])
    return factor_of


def normal_values(rng, dims, scale, limit, split=(), kind=jnp.bfloat16):
    drawn = jax.random.normal(rng, dims, jnp.float32) * scale
    if len(split) > 0:
        drawn = steps_of(rng, dims, split, -0.22, 0.18) * drawn
    return jnp.clip(drawn, min=-limit, max=limit).astype(kind)


def heavy_noise(rng, shape, spread, most, split, heavy, held_as=jnp.bfloat16):
    values = spread * jax.random.normal(rng, shape, jnp.float32)
    if split:
        values = values * steps_of(rng, shape, split, -0.22, 0.18)
    return jnp.clip(strengthened(values, jax.random.fold_in(rng, 3), *heavy), -most, most).astype(held_as)


def setup_inputs(seed: int = 0) -> dict:
    splits = jax.random.split(jax.random.key(seed), 4)
    deltas = heavy_noise(splits[0], (R, PROJ, D, FF), 0.5, 3.0, ((0, 4), (2, 8)), (0, 2, 4, 2.0))
    master = normal_values(splits[1], (PROJ, D, FF), 0.5, 3.0, ((1, 4), (2, 8)), jnp.float32)
    momentum = normal_values(splits[2], (PROJ, D, FF), 0.3, 2.0, ((1, 4), (2, 8)), jnp.float32)
    return {"deltas": deltas, "master": master, "momentum": momentum}


def reference(deltas, master, momentum):
    outer = jnp.sum(deltas.astype(jnp.float32), axis=0) / deltas.shape[0]
    velocity = 0.9 * momentum + outer
    updated = master - 0.7 * (outer + 0.9 * velocity)
    return updated, velocity, updated.astype(jnp.bfloat16)
```

```python
import functools

import jax
import jax.numpy as jnp
from jax import lax
from jax.experimental import pallas as pl
from jax.experimental.pallas import tpu as pltpu
from jax.sharding import PartitionSpec as P

F32, BF16 = jnp.float32, jnp.bfloat16
SPLITS = 4
AHEAD = 4
LAGS = (2, 5, 8, 10)


def kernel(
    dims, delta, master, momentum, master_out, momentum_out, out,
    own, half, cross, total, mas, mom,
    load, store, sent, pair_a, pair_b, cross_in, cross_side, total_in, back_in, side_in, last_in,
):
    R, F, PROJ, RB, FF, WD, H = dims
    B, X = F // R, R // PROJ
    RH, SUB, T = RB // X, WD // H, F * H
    w, f = lax.axis_index("replica"), lax.axis_index("fsdp")
    core, x = lax.rem(w, PROJ), w // PROJ
    a, b = f // B, lax.rem(f, B)
    other = 1 - core
    w_pair = x * PROJ + other
    w_side = (1 - x) * PROJ + core
    w_far = (1 - x) * PROJ + other
    pair, side = (w_pair, f), (w_side, f)
    near = x == a // PROJ
    far = jnp.logical_not(near)

    def turned(t):
        return lax.rem(t + t // F, 2) == 1

    def to(ref_src, ref_dst, send, recv, device):
        return pltpu.make_async_remote_copy(
            src_ref=ref_src, dst_ref=ref_dst, send_sem=send, recv_sem=recv,
            device_id=device, device_id_type=pl.DeviceIdType.MESH,
        )

    def block(worker, t):
        return lax.rem(lax.rem(t, F) + f + worker * B, F)

    def cols(worker, t):
        return pl.ds(pl.multiple_of(block(worker, t) * WD + (t // F) * SUB, 128), SUB)

    def rows(xi):
        return pl.ds(pl.multiple_of(xi * RH, RH), RH)

    def drain(ref, sem):
        pltpu.make_async_copy(ref, ref, sem).wait()

    barrier = pltpu.get_barrier_semaphore()
    mine = a == w

    def greet(device):
        pl.semaphore_signal(barrier, inc=1, device_id=device, device_id_type=pl.DeviceIdType.MESH)

    load_own = pltpu.make_async_copy(delta.at[core], own, load.at[0])
    load_mas = pltpu.make_async_copy(master, mas, load.at[1])
    load_mom = pltpu.make_async_copy(momentum, mom, load.at[2])
    load_own.start()
    load_mas.start()
    load_mom.start()
    greet(pair)
    greet(side)

    @pl.loop(0, F)
    def _(i):
        @pl.when(jnp.logical_not(jnp.logical_and(mine, i == f)))
        def _():
            greet((a, i))

        wi, bi = i // B, lax.rem(i, B)

        @pl.when(jnp.logical_not(jnp.logical_and(mine, jnp.logical_and(wi == w, bi == b))))
        def _():
            greet((wi, w * B + bi))

    @pl.when(mine)
    def _():
        pl.semaphore_wait(barrier, 2 * F)

    @pl.when(jnp.logical_not(mine))
    def _():
        pl.semaphore_wait(barrier, 2 * F + 2)

    def send_pair(t):
        cb, ca = cols(w_far, t), cols(w_pair, t)
        src = delta.at[other]
        to(src.at[rows(1 - x), cb], half.at[rows(1 - x), cb], sent.at[0], pair_b.at[t], pair).start()
        to(src.at[rows(x), ca], half.at[rows(x), ca], sent.at[0], pair_a.at[t], pair).start()

    def pair_sum(xi, c, arrived, send, recv):
        tile, mine_tile = half.at[rows(xi), c], own.at[rows(xi), c]
        pltpu.make_async_copy(tile, tile, arrived).wait()
        tile[...] = (tile[...].astype(F32) + mine_tile[...].astype(F32)).astype(BF16)
        to(tile, cross.at[rows(xi), c], send, recv, side).start()

    def step_cross(t):
        turn = turned(t)

        @pl.when(jnp.logical_not(jnp.logical_and(near, turn)))
        def _():
            pair_sum(1 - x, cols(w_side, t), pair_b.at[t], sent.at[1], cross_in.at[t])

        @pl.when(jnp.logical_and(far, turn))
        def _():
            pair_sum(x, cols(w, t), pair_a.at[t], sent.at[7], cross_side.at[t])

    def owner_slot(pi, bi, xi, t):
        return total.at[
            pi,
            pl.ds(pl.multiple_of(bi * RB + xi * RH, RH), RH),
            pl.ds(pl.multiple_of((t // F) * SUB, 128), SUB),
        ]

    def full_sum(worker, xi, t, arrived_pair, arrived_cross, send):
        c = cols(worker, t)
        tile, mine_tile, arrived = half.at[rows(xi), c], own.at[rows(xi), c], cross.at[rows(xi), c]
        pltpu.make_async_copy(tile, tile, arrived_pair).wait()
        pltpu.make_async_copy(arrived, arrived, arrived_cross).wait()
        tile[...] = (
            tile[...].astype(F32) + mine_tile[...].astype(F32) + arrived[...].astype(F32)
        ).astype(BF16)
        cb = block(worker, t)
        slot = owner_slot(core, b, xi, t)
        here = jnp.logical_and(mine, cb == f)

        @pl.when(here)
        def _():
            pltpu.make_async_copy(tile, slot, total_in.at[t]).start()

        @pl.when(jnp.logical_not(here))
        def _():
            to(tile, slot, send, total_in.at[t], (a, cb)).start()

    def step_total(t):
        turn = turned(t)

        @pl.when(jnp.logical_or(near, jnp.logical_not(turn)))
        def _():
            full_sum(w, x, t, pair_a.at[t], cross_in.at[t], sent.at[2])

        @pl.when(jnp.logical_and(near, turn))
        def _():
            full_sum(w_side, 1 - x, t, pair_b.at[t], cross_side.at[t], sent.at[6])

    def step_update(t):
        e = lax.rem(f + 2 * F - lax.rem(t, F) - w * B, F)
        we, be = e // B, lax.rem(e, B)
        pe, xe = lax.rem(we, PROJ), we // PROJ
        r0 = pl.multiple_of(be * RB + xe * RH, RH)
        rr = pl.ds(r0, RH)
        cc = pl.ds(pl.multiple_of((t // F) * SUB, 128), SUB)
        tile = owner_slot(pe, be, xe, t)
        pltpu.make_async_copy(tile, tile, total_in.at[t]).wait()
        m, v = mas.at[pe, rr, cc], mom.at[pe, rr, cc]
        outer = tile[...].astype(F32) / R
        velocity = 0.9 * v[...] + outer
        updated = m[...] - 0.7 * (outer + 0.9 * velocity)
        v[...] = velocity
        m[...] = updated
        tile[...] = updated.astype(BF16)
        pltpu.make_async_copy(m, master_out.at[pe, rr, cc], store.at[0]).start()
        pltpu.make_async_copy(v, momentum_out.at[pe, rr, cc], store.at[1]).start()
        fe = w * B + be
        dst = out.at[pe, rows(xe), pl.ds(pl.multiple_of(f * WD + (t // F) * SUB, 128), SUB)]
        here = jnp.logical_and(we == w, fe == f)

        @pl.when(here)
        def _():
            pltpu.make_async_copy(tile, dst, back_in.at[t]).start()

        @pl.when(jnp.logical_not(here))
        def _():
            to(tile, dst, sent.at[3], back_in.at[t], (we, fe)).start()

    def step_side(t):
        tile = out.at[core, rows(x), cols(w, t)]
        pltpu.make_async_copy(tile, tile, back_in.at[t]).wait()
        to(tile, tile, sent.at[4], side_in.at[t], side).start()
        to(tile, tile, sent.at[5], last_in, pair).start()

    def step_pair(t):
        tile = out.at[core, rows(1 - x), cols(w_side, t)]
        pltpu.make_async_copy(tile, tile, side_in.at[t]).wait()
        to(tile, tile, sent.at[5], last_in, pair).start()

    @pl.loop(0, min(AHEAD, T))
    def _(t):
        send_pair(t)

    load_own.wait()

    @pl.loop(0, T + LAGS[-1])
    def _(t):
        @pl.when(t + AHEAD < T)
        def _():
            send_pair(t + AHEAD)

        @pl.when(t < T)
        def _():
            step_cross(t)

        @pl.when(t == LAGS[1])
        def _():
            load_mas.wait()
            load_mom.wait()

        for lag, step in zip(LAGS, (step_total, step_update, step_side, step_pair)):
            @pl.when(jnp.logical_and(t >= lag, t < T + lag))
            def _():
                step(t - lag)

    drain(out.at[other], last_in)
    drain(half, sent.at[0])

    def drain_part(width, sem):
        drain(half.at[pl.ds(0, RH), pl.ds(0, width)], sem)

    @pl.when(mine)
    def _():
        drain_part(FF - WD, sent.at[2])
        drain_part((FF - WD) // 2, sent.at[6])
        drain_part(FF - WD, sent.at[3])

    @pl.when(jnp.logical_not(mine))
    def _():
        drain_part(FF, sent.at[3])

    @pl.when(jnp.logical_and(near, jnp.logical_not(mine)))
    def _():
        drain_part(FF, sent.at[2])
        drain_part(FF // 2, sent.at[6])

    @pl.when(near)
    def _():
        drain_part(FF // 2, sent.at[1])

    @pl.when(far)
    def _():
        drain_part(FF, sent.at[1])
        drain_part(FF // 2, sent.at[2])
        drain_part(FF // 2, sent.at[7])

    drain_part(FF, sent.at[4])
    drain(half, sent.at[5])
    drain(mas, store.at[0])
    drain(mom, store.at[1])


def on_device(deltas, master, momentum):
    local = deltas[0]
    R, F = lax.axis_size("replica"), lax.axis_size("fsdp")
    PROJ, RB, FF = local.shape
    WD = FF // F
    H = min(SPLITS, WD // 128)
    assert R == 2 * PROJ and PROJ == 2 and F % R == 0 and H % 2 == 0
    T = F * H
    hbm = pl.BlockSpec(memory_space=pl.ANY)
    dma = pltpu.SemaphoreType.DMA
    updated, velocity, params = pl.pallas_call(
        functools.partial(kernel, (R, F, PROJ, RB, FF, WD, H)),
        out_shape=(
            jax.ShapeDtypeStruct(master.shape, F32),
            jax.ShapeDtypeStruct(momentum.shape, F32),
            jax.ShapeDtypeStruct(local.shape, BF16),
        ),
        in_specs=[hbm] * 3,
        out_specs=(hbm,) * 3,
        scratch_shapes=[
            pltpu.VMEM((RB, FF), BF16),
            pltpu.VMEM((RB, FF), BF16),
            pltpu.VMEM((RB, FF), BF16),
            pltpu.VMEM(master.shape, BF16),
            pltpu.VMEM(master.shape, F32),
            pltpu.VMEM(master.shape, F32),
            dma((3,)), dma((2,)), dma((8,)),
            dma((T,)), dma((T,)), dma((T,)), dma((T,)), dma((T,)), dma((T,)), dma((T,)), dma,
        ],
        compiler_params=pltpu.CompilerParams(
            collective_id=0, has_side_effects=True, vmem_limit_bytes=56 * 2**20
        ),
    )(local, master, momentum)
    return updated, velocity, params


def solution(mesh):
    return jax.shard_map(
        on_device,
        mesh=mesh,
        in_specs=(
            P("replica", None, "fsdp", None),
            P(None, "replica", "fsdp"),
            P(None, "replica", "fsdp"),
        ),
        out_specs=(P(None, "replica", "fsdp"), P(None, "replica", "fsdp"), P(None, "fsdp", None)),
        check_vma=False,
    )
```
